16 devices in a mesh: col: 4 (over z, y), row: 4 (over x, core).
Axes of the slice: x: 2, y: 2, z: 2, core: 2. Of those that a mesh axis runs over, the one named last changes fastest.
Arguments:
- matrix: bfloat16 [12288, 12288], P('row', 'col')
- y_start: float32 [12288, 32], P(('col', 'row'))
- center: float32 [], replicated
- half_width: float32 [], replicated
Outputs:
- output 1: float32 [12288, 32], P(('col', 'row'))
- output 2: float32 [32, 32], replicated
All inputs are finite; a program needn't handle non-finite values.
Results may differ from the reference program's by a relative error of at most 0.012416.
Values are sent between devices in bfloat16 or wider.
A program may use at most 1 GiB of HBM per device.

```python
import jax
import jax.numpy as jnp
from jax import lax

N = 12288
WIDTH = 32
DEGREE = 8


def setup_inputs(seed: int = 0) -> dict:
    root_key = jax.random.key(seed)
    key_mat, key_vec, key_center, key_width = jax.random.split(root_key, 4)
    base_draw = jax.random.normal(key_mat, (N, N), jnp.float32)
    matrix = ((base_draw + base_draw.T) * (2.0 * N) ** -0.5).astype(jnp.bfloat16)
    y_start = jax.random.normal(key_vec, (N, WIDTH), jnp.float32)
    center = jax.random.uniform(key_center, (), jnp.float32, -0.5, 0.5)
    half_width = 2.3 + jnp.abs(center) + jax.random.uniform(key_width, (), jnp.float32, 0.0, 0.5)
    return {"matrix": matrix, "y_start": y_start, "center": center, "half_width": half_width}


def apply_matrix(matrix, vectors):
    return jnp.dot(matrix, vectors.astype(jnp.bfloat16), preferred_element_type=jnp.float32)


def reference(matrix, y_start, center, half_width):
    y_first = (apply_matrix(matrix, y_start) - center * y_start) / half_width

    def sweep_step(state_pair, unused):
        y_prev, y_cur = state_pair
        y_next = 2.0 * (apply_matrix(matrix, y_cur) - center * y_cur) / half_width - y_prev
        return (y_cur, y_next), unused

    final_pair, unused_out = lax.scan(sweep_step, (y_start, y_first), None, length=DEGREE - 1)
    y_last = final_pair[1]
    y_low = y_last.astype(jnp.bfloat16)
    image_low = apply_matrix(matrix, y_last).astype(jnp.bfloat16)
    gram_mat = jnp.dot(y_low.T, image_low, preferred_element_type=jnp.float32) / N
    return y_last, gram_mat
```

```python
import functools

import jax
import jax.numpy as jnp
from jax import lax
from jax.experimental import pallas as pl
from jax.experimental.pallas import tpu as pltpu
from jax.sharding import PartitionSpec as P

DEGREE = 8
MESH = pl.DeviceIdType.MESH


def filter_kernel(rows, cols, a_hbm, y_in, c_in, e_in, y_out, g_out, a_v, part, y_cur, y_prev, y_send, y_got, pair_got, x_got, g_send, g_got,
                  a_sem, gat_send, gat_recv, pair_send, pair_recv, x_send, x_recv, g_ssem, g_rsem):
    i = lax.axis_index("row")
    j = lax.axis_index("col")
    width, piece = y_in.shape
    n_all = piece * rows * cols

    def block_copy(kq, nq):
        src_rows = pl.ds(pl.multiple_of((i ^ kq) * piece, piece), piece)
        src_cols = pl.ds(pl.multiple_of((i ^ nq) * piece, piece), piece)
        return pltpu.make_async_copy(a_hbm.at[src_rows, src_cols], a_v.at[nq, kq], a_sem.at[kq, nq])

    order = (3, 2, 1, 0)
    for kq in range(4):
        for nq in order:
            block_copy(kq, nq).start()

    barrier = pltpu.get_barrier_semaphore()
    for dr in range(rows):
        for dc in range(cols):
            if dr or dc:
                pl.semaphore_signal(barrier, inc=1, device_id={"row": i ^ dr, "col": j ^ dc}, device_id_type=MESH)
    pl.semaphore_wait(barrier, rows * cols - 1)

    center = c_in[0, 0]
    half_width = e_in[0, 0]
    y_cur[...] = y_in[...]
    y_prev[...] = jnp.zeros_like(y_prev)
    y_send[...] = y_in[...].astype(jnp.bfloat16)

    def gather_copy(dc, par):
        return pltpu.make_async_remote_copy(
            src_ref=y_send, dst_ref=y_got.at[par, i ^ j], send_sem=gat_send.at[dc], recv_sem=gat_recv.at[par, i ^ j],
            device_id={"row": j, "col": j ^ dc}, device_id_type=MESH)

    def gather_arrival(kq, par):
        return pltpu.make_async_remote_copy(
            src_ref=y_send, dst_ref=y_got.at[par, kq], send_sem=gat_send.at[0], recv_sem=gat_recv.at[par, kq],
            device_id={"row": j, "col": j ^ 1}, device_id_type=MESH)

    def pair_copy(q, par):
        return pltpu.make_async_remote_copy(
            src_ref=part.at[2 * q + 1], dst_ref=pair_got.at[par, q], send_sem=pair_send.at[q], recv_sem=pair_recv.at[par, q],
            device_id={"row": i ^ 1, "col": j}, device_id_type=MESH)

    def x_copy(par):
        return pltpu.make_async_remote_copy(
            src_ref=part.at[2], dst_ref=x_got.at[par], send_sem=x_send, recv_sem=x_recv.at[par],
            device_id={"row": i ^ 2, "col": j}, device_id_type=MESH)

    def apply(t, first):
        par = lax.rem(t, 2)

        @pl.when(i != j)
        def _():
            gather_copy(0, par).start()

        @pl.when(i == j)
        def _():
            y_got[par, 0] = y_send[...]

        for dc in (3, 2, 1):
            gather_copy(dc, par).start()

        for kq in range(4):
            if kq == 0:
                @pl.when(i != j)
                def _():
                    gather_arrival(0, par).wait_recv()
            else:
                gather_arrival(kq, par).wait_recv()
            for nq in order:
                if first:
                    block_copy(kq, nq).wait()
                prod = jnp.dot(y_got[par, kq], a_v[nq, kq], preferred_element_type=jnp.float32)
                part[nq] = prod if kq == 0 else part[nq] + prod
                if kq == 3 and nq % 2 == 1:
                    pair_copy(nq // 2, par).start()

        pair_copy(1, par).wait_recv()
        part[2] = part[2] + pair_got[par, 1]
        x_copy(par).start()
        pair_copy(0, par).wait_recv()
        own = part[0] + pair_got[par, 0]
        x_copy(par).wait_recv()
        image = own + x_got[par]

        @pl.when(i != j)
        def _():
            gather_copy(0, par).wait_send()

        for dc in (3, 2, 1):
            gather_copy(dc, par).wait_send()
        pair_copy(1, par).wait_send()
        pair_copy(0, par).wait_send()
        x_copy(par).wait_send()
        return image

    def advance(t, factor, image):
        y_next = factor * (image - center * y_cur[...]) / half_width - y_prev[...]
        y_prev[...] = y_cur[...]
        y_cur[...] = y_next
        y_send[...] = y_next.astype(jnp.bfloat16)

    advance(0, 1.0, apply(0, True))

    def step(t, carry):
        advance(t, 2.0, apply(t, False))
        return carry

    lax.fori_loop(1, DEGREE, step, 0)
    y_out[...] = y_cur[...]
    image_low = apply(DEGREE, False).astype(jnp.bfloat16)
    gram = lax.dot_general(y_send[...], image_low, (((1,), (1,)), ((), ())), preferred_element_type=jnp.float32)
    strip = width // 4
    g_send[...] = jnp.concatenate([gram[strip * s: strip * (s + 1)] for s in range(4)], axis=1)
    me = i * cols + j

    def gram_copy(dr, dc):
        idx = dr * cols + dc
        return pltpu.make_async_remote_copy(
            src_ref=g_send, dst_ref=g_got.at[me], send_sem=g_ssem.at[idx], recv_sem=g_rsem.at[me],
            device_id={"row": i ^ dr, "col": j ^ dc}, device_id_type=MESH)

    def gram_arrival(dr, dc):
        src = (i ^ dr) * cols + (j ^ dc)
        return pltpu.make_async_remote_copy(
            src_ref=g_send, dst_ref=g_got.at[src], send_sem=g_ssem.at[0], recv_sem=g_rsem.at[src],
            device_id={"row": i ^ dr, "col": j ^ dc}, device_id_type=MESH)

    pairs = [(dr, dc) for dr in range(rows) for dc in range(cols) if dr or dc]
    for dr, dc in reversed(pairs):
        gram_copy(dr, dc).start()
    g_got[me] = g_send[...]
    for dr, dc in pairs:
        gram_arrival(dr, dc).wait_recv()
    total = g_got[0]
    for k in range(1, rows * cols):
        total = total + g_got[k]
    total = total / n_all
    for s in range(4):
        g_out[strip * s: strip * (s + 1), :] = total[:, width * s: width * (s + 1)]
    for dr, dc in pairs:
        gram_copy(dr, dc).wait_send()


def solution(mesh):
    rows = mesh.shape["row"]
    cols = mesh.shape["col"]
    both_axes = ("col", "row")

    def local_filter(mat_tile, y_start, center, half_width):
        piece, width = y_start.shape
        f32, bf16 = jnp.float32, jnp.bfloat16
        dma = pltpu.SemaphoreType.DMA
        strip = width // 4
        y_t, gram = pl.pallas_call(
            functools.partial(filter_kernel, rows, cols),
            out_shape=(jax.ShapeDtypeStruct((width, piece), f32), jax.ShapeDtypeStruct((width, width), f32)),
            in_specs=[pl.BlockSpec(memory_space=pltpu.HBM), pl.BlockSpec(memory_space=pltpu.VMEM),
                      pl.BlockSpec(memory_space=pltpu.SMEM), pl.BlockSpec(memory_space=pltpu.SMEM)],
            out_specs=(pl.BlockSpec(memory_space=pltpu.VMEM), pl.BlockSpec(memory_space=pltpu.VMEM)),
            scratch_shapes=[
                pltpu.VMEM((4, 4, piece, piece), bf16),
                pltpu.VMEM((4, width, piece), f32),
                pltpu.VMEM((width, piece), f32),
                pltpu.VMEM((width, piece), f32),
                pltpu.VMEM((width, piece), bf16),
                pltpu.VMEM((2, 4, width, piece), bf16),
                pltpu.VMEM((2, 2, width, piece), f32),
                pltpu.VMEM((2, width, piece), f32),
                pltpu.VMEM((strip, 4 * width), f32),
                pltpu.VMEM((rows * cols, strip, 4 * width), f32),
                dma((4, 4)), dma((4,)), dma((2, 4)), dma((2,)), dma((2, 2)), dma, dma((2,)),
                dma((rows * cols,)), dma((rows * cols,)),
            ],
            compiler_params=pltpu.CompilerParams(collective_id=0, has_side_effects=True, vmem_limit_bytes=56 * 1024 * 1024),
        )(mat_tile, y_start.T, center.reshape(1, 1), half_width.reshape(1, 1))
        return y_t.T, gram

    return jax.shard_map(local_filter, mesh=mesh, in_specs=(P("row", "col"), P(both_axes, None), P(), P()),
                         out_specs=(P(both_axes, None), P()), check_vma=False)
```

```python
import functools

import jax
import jax.numpy as jnp
from jax import lax
from jax.experimental import pallas as pl
from jax.experimental.pallas import tpu as pltpu
from jax.sharding import PartitionSpec as P

DEGREE = 8
CHUNK = 256
MESH = pl.DeviceIdType.MESH


def filter_kernel(rows, cols, a_hbm, y_in, c_in, e_in, y_out, g_out, a_v, part, y_cur, y_prev, y_send, y_got, pair_got, x_got, g_send, g_got,
                  a_sem, gat_send, gat_recv, pair_send, pair_recv, x_send, x_recv, g_ssem, g_rsem):
    i = lax.axis_index("row")
    j = lax.axis_index("col")
    width, piece = y_in.shape
    n_all = piece * rows * cols
    chunks = piece // CHUNK
    slots = (3, 1, 2, 0)

    def block_copy(h, n, kq):
        src_rows = pl.ds(pl.multiple_of((i ^ kq) * piece + h * CHUNK, CHUNK), CHUNK)
        src_cols = pl.ds(pl.multiple_of((i ^ slots[n]) * piece, piece), piece)
        return pltpu.make_async_copy(a_hbm.at[src_rows, src_cols], a_v.at[h, n, pl.ds(kq * CHUNK, CHUNK)], a_sem.at[h, n])

    for h in range(chunks):
        for n in range(4):
            for kq in range(4):
                block_copy(h, n, kq).start()

    def block_wait(h, n):
        pltpu.make_async_copy(a_hbm.at[pl.ds(0, 4 * CHUNK), pl.ds(0, piece)], a_v.at[h, n], a_sem.at[h, n]).wait()

    barrier = pltpu.get_barrier_semaphore()
    for dr in range(rows):
        for dc in range(cols):
            if dr or dc:
                pl.semaphore_signal(barrier, inc=1, device_id={"row": i ^ dr, "col": j ^ dc}, device_id_type=MESH)
    pl.semaphore_wait(barrier, rows * cols - 1)

    center = c_in[0, 0]
    half_width = e_in[0, 0]

    def gather_copy(dc, g, par):
        return pltpu.make_async_remote_copy(
            src_ref=y_send.at[g], dst_ref=y_got.at[par, g, i ^ j], send_sem=gat_send.at[g, dc], recv_sem=gat_recv.at[par, g, i ^ j],
            device_id={"row": j, "col": j ^ dc}, device_id_type=MESH)

    def gather_arrival(kq, g, par):
        return pltpu.make_async_remote_copy(
            src_ref=y_send.at[g], dst_ref=y_got.at[par, g, kq], send_sem=gat_send.at[g, 0], recv_sem=gat_recv.at[par, g, kq],
            device_id={"row": j, "col": j ^ 1}, device_id_type=MESH)

    def pair_copy(g, par):
        return pltpu.make_async_remote_copy(
            src_ref=part.at[g, pl.ds(0, 2)], dst_ref=pair_got.at[par, g], send_sem=pair_send.at[g], recv_sem=pair_recv.at[par, g],
            device_id={"row": i ^ 1, "col": j}, device_id_type=MESH)

    def x_copy(g, par):
        return pltpu.make_async_remote_copy(
            src_ref=part.at[g, 2], dst_ref=x_got.at[par, g], send_sem=x_send.at[g], recv_sem=x_recv.at[par, g],
            device_id={"row": i ^ 2, "col": j}, device_id_type=MESH)

    def gather_start(g, par):
        @pl.when(i != j)
        def _():
            gather_copy(0, g, par).start()

        @pl.when(i == j)
        def _():
            y_got[par, g, 0] = y_send[g]

        for dc in (3, 2, 1):
            gather_copy(dc, g, par).start()

    def gather_sent(g, par):
        @pl.when(i != j)
        def _():
            gather_copy(0, g, par).wait_send()

        for dc in (3, 2, 1):
            gather_copy(dc, g, par).wait_send()

    def source(h, par):
        @pl.when(i != j)
        def _():
            gather_arrival(0, h, par).wait_recv()

        for kq in (1, 2, 3):
            gather_arrival(kq, h, par).wait_recv()
        return jnp.concatenate([y_got[par, h, kq] for kq in range(4)], axis=1)

    def apply(par, first, consume):
        for h in range(chunks):
            lhs = source(h, par)
            if first:
                for n in range(4):
                    block_wait(h, n)
            for g in range(chunks):
                for n in range(4):
                    prod = jnp.dot(lhs, a_v[h, n, :, CHUNK * g: CHUNK * (g + 1)], preferred_element_type=jnp.float32)
                    part[g, n] = prod if h == 0 else part[g, n] + prod
                if h == chunks - 1:
                    pair_copy(g, par).start()
        for g in range(chunks):
            pair_copy(g, par).wait_recv()
            part[g, 2] = part[g, 2] + pair_got[par, g, 0]
            x_copy(g, par).start()
        for g in range(chunks):
            own = part[g, 3] + pair_got[par, g, 1]
            x_copy(g, par).wait_recv()
            consume(g, own + x_got[par, g])
        for g in range(chunks):
            pair_copy(g, par).wait_send()
            x_copy(g, par).wait_send()

    def advance(par, factor):
        def consume(g, image):
            y_now = y_cur[g]
            y_next = factor * (image - center * y_now) / half_width - y_prev[g]
            y_prev[g] = y_now
            y_cur[g] = y_next
            gather_sent(g, par)
            y_send[g] = y_next.astype(jnp.bfloat16)
            gather_start(g, 1 - par)
        return consume

    for g in range(chunks):
        y_now = y_in[:, CHUNK * g: CHUNK * (g + 1)]
        y_cur[g] = y_now
        y_prev[g] = jnp.zeros_like(y_now)
        y_send[g] = y_now.astype(jnp.bfloat16)
        gather_start(g, 0)
    apply(0, True, advance(0, 1.0))

    def step(t, carry):
        par = lax.rem(t, 2)
        apply(par, False, advance(par, 2.0))
        return carry

    lax.fori_loop(1, DEGREE, step, 0)
    for g in range(chunks):
        y_out[:, CHUNK * g: CHUNK * (g + 1)] = y_cur[g]
    images = []
    apply(DEGREE % 2, False, lambda g, image: images.append(image.astype(jnp.bfloat16)))
    for g in range(chunks):
        gather_sent(g, DEGREE % 2)
    image_low = jnp.concatenate(images, axis=1)
    y_low = jnp.concatenate([y_send[g] for g in range(chunks)], axis=1)
    gram = lax.dot_general(y_low, image_low, (((1,), (1,)), ((), ())), preferred_element_type=jnp.float32)
    strip = width // 4
    g_send[...] = jnp.concatenate([gram[strip * s: strip * (s + 1)] for s in range(4)], axis=1)
    me = i * cols + j

    def gram_copy(dr, dc):
        idx = dr * cols + dc
        return pltpu.make_async_remote_copy(
            src_ref=g_send, dst_ref=g_got.at[me], send_sem=g_ssem.at[idx], recv_sem=g_rsem.at[me],
            device_id={"row": i ^ dr, "col": j ^ dc}, device_id_type=MESH)

    def gram_arrival(dr, dc):
        src = (i ^ dr) * cols + (j ^ dc)
        return pltpu.make_async_remote_copy(
            src_ref=g_send, dst_ref=g_got.at[src], send_sem=g_ssem.at[0], recv_sem=g_rsem.at[src],
            device_id={"row": i ^ dr, "col": j ^ dc}, device_id_type=MESH)

    pairs = [(dr, dc) for dr in range(rows) for dc in range(cols) if dr or dc]
    for dr, dc in reversed(pairs):
        gram_copy(dr, dc).start()
    g_got[me] = g_send[...]
    for dr, dc in pairs:
        gram_arrival(dr, dc).wait_recv()
    total = g_got[0]
    for k in range(1, rows * cols):
        total = total + g_got[k]
    total = total / n_all
    for s in range(4):
        g_out[strip * s: strip * (s + 1), :] = total[:, width * s: width * (s + 1)]
    for dr, dc in pairs:
        gram_copy(dr, dc).wait_send()


def solution(mesh):
    rows = mesh.shape["row"]
    cols = mesh.shape["col"]
    both_axes = ("col", "row")

    def local_filter(mat_tile, y_start, center, half_width):
        piece, width = y_start.shape
        f32, bf16 = jnp.float32, jnp.bfloat16
        dma = pltpu.SemaphoreType.DMA
        strip = width // 4
        chunks = piece // CHUNK
        y_t, gram = pl.pallas_call(
            functools.partial(filter_kernel, rows, cols),
            out_shape=(jax.ShapeDtypeStruct((width, piece), f32), jax.ShapeDtypeStruct((width, width), f32)),
            in_specs=[pl.BlockSpec(memory_space=pltpu.HBM), pl.BlockSpec(memory_space=pltpu.VMEM),
                      pl.BlockSpec(memory_space=pltpu.SMEM), pl.BlockSpec(memory_space=pltpu.SMEM)],
            out_specs=(pl.BlockSpec(memory_space=pltpu.VMEM), pl.BlockSpec(memory_space=pltpu.VMEM)),
            scratch_shapes=[
                pltpu.VMEM((chunks, 4, 4 * CHUNK, piece), bf16),
                pltpu.VMEM((chunks, 4, width, CHUNK), f32),
                pltpu.VMEM((chunks, width, CHUNK), f32),
                pltpu.VMEM((chunks, width, CHUNK), f32),
                pltpu.VMEM((chunks, width, CHUNK), bf16),
                pltpu.VMEM((2, chunks, 4, width, CHUNK), bf16),
                pltpu.VMEM((2, chunks, 2, width, CHUNK), f32),
                pltpu.VMEM((2, chunks, width, CHUNK), f32),
                pltpu.VMEM((strip, 4 * width), f32),
                pltpu.VMEM((rows * cols, strip, 4 * width), f32),
                dma((chunks, 4)), dma((chunks, 4)), dma((2, chunks, 4)), dma((chunks,)), dma((2, chunks)), dma((chunks,)), dma((2, chunks)),
                dma((rows * cols,)), dma((rows * cols,)),
            ],
            compiler_params=pltpu.CompilerParams(collective_id=0, has_side_effects=True, vmem_limit_bytes=56 * 1024 * 1024),
        )(mat_tile, y_start.T, center.reshape(1, 1), half_width.reshape(1, 1))
        return y_t.T, gram

    return jax.shard_map(local_filter, mesh=mesh, in_specs=(P("row", "col"), P(both_axes, None), P(), P()),
                         out_specs=(P(both_axes, None), P()), check_vma=False)
```

```python
import functools

import jax
import jax.numpy as jnp
from jax import lax
from jax.experimental import pallas as pl
from jax.experimental.pallas import tpu as pltpu
from jax.sharding import PartitionSpec as P

DEGREE = 8
CHUNK = 128
MESH = pl.DeviceIdType.MESH


def filter_kernel(rows, cols, a_hbm, y_in, c_in, e_in, y_out, g_out, a_v, part, y_cur, y_prev, y_send, y_got, pair_got, x_got, g_send, g_got,
                  a_sem, gat_send, gat_recv, pair_send, pair_recv, x_send, x_recv, g_ssem, g_rsem):
    i = lax.axis_index("row")
    j = lax.axis_index("col")
    width, piece = y_in.shape
    n_all = piece * rows * cols
    chunks = piece // CHUNK
    slots = (2, 1, 3, 0)

    def block_copy(h, n, kq):
        src_rows = pl.ds(pl.multiple_of((i ^ kq) * piece + h * CHUNK, CHUNK), CHUNK)
        src_cols = pl.ds(pl.multiple_of((i ^ slots[n]) * piece, piece), piece)
        return pltpu.make_async_copy(a_hbm.at[src_rows, src_cols], a_v.at[h, n, pl.ds(kq * CHUNK, CHUNK)], a_sem.at[h, n])

    for h in range(chunks):
        for n in range(4):
            for kq in range(4):
                block_copy(h, n, kq).start()

    def block_wait(h, n):
        pltpu.make_async_copy(a_hbm.at[pl.ds(0, 4 * CHUNK), pl.ds(0, piece)], a_v.at[h, n], a_sem.at[h, n]).wait()

    barrier = pltpu.get_barrier_semaphore()
    for dr in range(rows):
        for dc in range(cols):
            if dr or dc:
                pl.semaphore_signal(barrier, inc=1, device_id={"row": i ^ dr, "col": j ^ dc}, device_id_type=MESH)
    pl.semaphore_wait(barrier, rows * cols - 1)

    center = c_in[0, 0]
    half_width = e_in[0, 0]

    def gather_copy(dc, g, par):
        return pltpu.make_async_remote_copy(
            src_ref=y_send.at[g], dst_ref=y_got.at[par, g, i ^ j], send_sem=gat_send.at[g], recv_sem=gat_recv.at[par, g],
            device_id={"row": j, "col": j ^ dc}, device_id_type=MESH)

    def pair_copy(g, par):
        return pltpu.make_async_remote_copy(
            src_ref=part.at[g, pl.ds(0, 2)], dst_ref=pair_got.at[par, g], send_sem=pair_send.at[g], recv_sem=pair_recv.at[par, g],
            device_id={"row": i ^ 1, "col": j}, device_id_type=MESH)

    def x_copy(g, par):
        return pltpu.make_async_remote_copy(
            src_ref=part.at[g, 2], dst_ref=x_got.at[par, g], send_sem=x_send.at[g], recv_sem=x_recv.at[par, g],
            device_id={"row": i ^ 3, "col": j}, device_id_type=MESH)

    def gather_start(g, par):
        for dc in (3, 2, 1):
            gather_copy(dc, g, par).start()

        @pl.when(i != j)
        def _():
            gather_copy(0, g, par).start()

        @pl.when(i == j)
        def _():
            y_got[par, g, 0] = y_send[g]

    def four_blocks(g, par, count):
        ref = y_got.at[par, g, pl.ds(0, count)]
        return pltpu.make_async_remote_copy(
            src_ref=ref, dst_ref=ref, send_sem=gat_send.at[g], recv_sem=gat_recv.at[par, g],
            device_id={"row": i, "col": j ^ 1}, device_id_type=MESH)

    def gather_sent(g, par):
        @pl.when(i != j)
        def _():
            four_blocks(g, par, 4).wait_send()

        @pl.when(i == j)
        def _():
            four_blocks(g, par, 3).wait_send()

    def source(h, par):
        @pl.when(i != j)
        def _():
            four_blocks(h, par, 4).wait_recv()

        @pl.when(i == j)
        def _():
            four_blocks(h, par, 3).wait_recv()

        return jnp.concatenate([y_got[par, h, kq] for kq in range(4)], axis=1)

    def apply(par, first, consume):
        for h in range(chunks):
            lhs = source(h, par)
            if first:
                for n in range(4):
                    block_wait(h, n)
            for g in range(chunks):
                tile = jnp.concatenate([a_v[h, n, :, CHUNK * g: CHUNK * (g + 1)] for n in range(4)], axis=1)
                prod = jnp.dot(lhs, tile, preferred_element_type=jnp.float32)
                for n in range(4):
                    term = prod[:, CHUNK * n: CHUNK * (n + 1)]
                    part[g, n] = term if h == 0 else part[g, n] + term
                if h == chunks - 1:
                    pair_copy(g, par).start()
        for g in range(chunks):
            pair_copy(g, par).wait_recv()
            part[g, 2] = part[g, 2] + pair_got[par, g, 0]
            x_copy(g, par).start()
        for g in range(chunks):
            own = part[g, 3] + pair_got[par, g, 1]
            x_copy(g, par).wait_recv()
            consume(g, own + x_got[par, g])
        for g in range(chunks):
            pair_copy(g, par).wait_send()
            x_copy(g, par).wait_send()

    def advance(par, factor):
        def consume(g, image):
            y_now = y_cur[g]
            y_next = factor * (image - center * y_now) / half_width - y_prev[g]
            y_prev[g] = y_now
            y_cur[g] = y_next
            gather_sent(g, par)
            y_send[g] = y_next.astype(jnp.bfloat16)
            gather_start(g, 1 - par)
        return consume

    for g in range(chunks):
        y_now = y_in[:, CHUNK * g: CHUNK * (g + 1)]
        y_cur[g] = y_now
        y_prev[g] = jnp.zeros_like(y_now)
        y_send[g] = y_now.astype(jnp.bfloat16)
        gather_start(g, 0)
    apply(0, True, advance(0, 1.0))

    def step(t, carry):
        par = lax.rem(t, 2)
        apply(par, False, advance(par, 2.0))
        return carry

    lax.fori_loop(1, DEGREE, step, 0)
    for g in range(chunks):
        y_out[:, CHUNK * g: CHUNK * (g + 1)] = y_cur[g]
    images = []
    apply(DEGREE % 2, False, lambda g, image: images.append(image.astype(jnp.bfloat16)))
    for g in range(chunks):
        gather_sent(g, DEGREE % 2)
    image_low = jnp.concatenate(images, axis=1)
    y_low = jnp.concatenate([y_send[g] for g in range(chunks)], axis=1)
    gram = lax.dot_general(y_low, image_low, (((1,), (1,)), ((), ())), preferred_element_type=jnp.float32)
    strip = width // 4
    g_send[...] = jnp.concatenate([gram[strip * s: strip * (s + 1)] for s in range(4)], axis=1)
    me = i * cols + j

    def gram_copy(dr, dc):
        idx = dr * cols + dc
        return pltpu.make_async_remote_copy(
            src_ref=g_send, dst_ref=g_got.at[me], send_sem=g_ssem.at[idx], recv_sem=g_rsem.at[me],
            device_id={"row": i ^ dr, "col": j ^ dc}, device_id_type=MESH)

    def gram_arrival(dr, dc):
        src = (i ^ dr) * cols + (j ^ dc)
        return pltpu.make_async_remote_copy(
            src_ref=g_send, dst_ref=g_got.at[src], send_sem=g_ssem.at[0], recv_sem=g_rsem.at[src],
            device_id={"row": i ^ dr, "col": j ^ dc}, device_id_type=MESH)

    pairs = [(dr, dc) for dr in range(rows) for dc in range(cols) if dr or dc]
    for dr, dc in reversed(pairs):
        gram_copy(dr, dc).start()
    g_got[me] = g_send[...]
    for dr, dc in pairs:
        gram_arrival(dr, dc).wait_recv()
    total = g_got[0]
    for k in range(1, rows * cols):
        total = total + g_got[k]
    total = total / n_all
    for s in range(4):
        g_out[strip * s: strip * (s + 1), :] = total[:, width * s: width * (s + 1)]
    for dr, dc in pairs:
        gram_copy(dr, dc).wait_send()


def solution(mesh):
    rows = mesh.shape["row"]
    cols = mesh.shape["col"]
    both_axes = ("col", "row")

    def local_filter(mat_tile, y_start, center, half_width):
        piece, width = y_start.shape
        f32, bf16 = jnp.float32, jnp.bfloat16
        dma = pltpu.SemaphoreType.DMA
        strip = width // 4
        chunks = piece // CHUNK
        y_t, gram = pl.pallas_call(
            functools.partial(filter_kernel, rows, cols),
            out_shape=(jax.ShapeDtypeStruct((width, piece), f32), jax.ShapeDtypeStruct((width, width), f32)),
            in_specs=[pl.BlockSpec(memory_space=pltpu.HBM), pl.BlockSpec(memory_space=pltpu.VMEM),
                      pl.BlockSpec(memory_space=pltpu.SMEM), pl.BlockSpec(memory_space=pltpu.SMEM)],
            out_specs=(pl.BlockSpec(memory_space=pltpu.VMEM), pl.BlockSpec(memory_space=pltpu.VMEM)),
            scratch_shapes=[
                pltpu.VMEM((chunks, 4, 4 * CHUNK, piece), bf16),
                pltpu.VMEM((chunks, 4, width, CHUNK), f32),
                pltpu.VMEM((chunks, width, CHUNK), f32),
                pltpu.VMEM((chunks, width, CHUNK), f32),
                pltpu.VMEM((chunks, width, CHUNK), bf16),
                pltpu.VMEM((2, chunks, 4, width, CHUNK), bf16),
                pltpu.VMEM((2, chunks, 2, width, CHUNK), f32),
                pltpu.VMEM((2, chunks, width, CHUNK), f32),
                pltpu.VMEM((strip, 4 * width), f32),
                pltpu.VMEM((rows * cols, strip, 4 * width), f32),
                dma((chunks, 4)), dma((chunks,)), dma((2, chunks)), dma((chunks,)), dma((2, chunks)), dma((chunks,)), dma((2, chunks)),
                dma((rows * cols,)), dma((rows * cols,)),
            ],
            compiler_params=pltpu.CompilerParams(collective_id=0, has_side_effects=True, vmem_limit_bytes=56 * 1024 * 1024),
        )(mat_tile, y_start.T, center.reshape(1, 1), half_width.reshape(1, 1))
        return y_t.T, gram

    return jax.shard_map(local_filter, mesh=mesh, in_specs=(P("row", "col"), P(both_axes, None), P(), P()),
                         out_specs=(P(both_axes, None), P()), check_vma=False)
```
